512 devices in a mesh: sx: 32 (over z_hi, x, core), sy: 16 (over z_lo, y).
Axes of the slice: x: 4, y: 8, z: 8 (z_hi: 4, z_lo: 2; z = z_hi * 2 + z_lo), core: 2. Of those that a mesh axis runs over, the one named last changes fastest.
Arguments:
- sources: bfloat16 [32, 16, 2, 64, 4096], P('sx', 'sy'), may hold values from -6 to 6
- translate_re: bfloat16 [4, 2, 2, 64, 64], replicated, may hold values from -0.375 to 0.375
- translate_im: bfloat16 [4, 2, 2, 64, 64], replicated, may hold values from -0.375 to 0.375
- frame_index: int32 [32, 16, 16], P('sx', 'sy'), may hold values from 0 to 4095
- velocity_index: int32 [32, 16, 256], P('sx', 'sy'), may hold values from 0 to 4095
- eval_re: bfloat16 [64, 64], replicated, may hold values from -1.5 to 1.5
- eval_im: bfloat16 [64, 64], replicated, may hold values from -1.5 to 1.5
- window: int32 [32, 16], P('sx', 'sy'), may hold values from 1 to 2
Outputs:
- smoothed: bfloat16 [256, 128, 4096], P('sx', 'sy')
The draws below stay inside these ranges and needn't reach their ends.
All inputs are finite; a program needn't handle non-finite values.
Results may differ from the reference program's by a relative error of at most 0.0076.
Values may be sent and summed in bfloat16 or wider, within the bound.
No kernel may reach another device: no remote copies, remote signals or barrier semaphores. Data moves between devices by JAX's collectives and lax.ppermute only.
A program may use at most 64 MiB of HBM per device.

```python
import math
import jax
import jax.numpy as jnp
from jax import lax

K = 64
TILE = 8
LEVELS = 4
FRAMES = 16
VGRID = 4096
VEL_DEV = 256
COLS = 4096
PX = 32
PY = 16
TX = 256
TY = 128
N_SX = 32
N_SY = 16


def plant(result, stream_key, low, top_value):
    longest = result.shape.index(max(result.shape))
    spots = []
    for shift in (0, 1):
        where = [jax.random.randint(jax.random.fold_in(stream_key, axis), (), 0, length) for axis, length in enumerate(result.shape)]
        where[longest] = (where[longest] + shift) % result.shape[longest]
        spots.append(tuple(where))
    return result.at[spots[0]].set(low).at[spots[1]].set(top_value)


def levels(stream_key, shape, cuts, low, top_value):
    gain = 1.0
    for dim, parts in cuts:
        draws = jax.random.uniform(jax.random.fold_in(jax.random.fold_in(stream_key, 6), dim), (parts,), jnp.float32, low / len(cuts), top_value / len(cuts))
        gain = gain * jnp.repeat(jnp.exp(draws), shape[dim] // parts).reshape((-1,) + (1,) * (len(shape) - 1 - dim))
    return gain


def gaussian(rng, shape, scale, most, shards=(), kind=jnp.bfloat16):
    gain = levels(rng, shape, shards, -0.22, 0.18) if shards else 1.0
    drawn = jax.random.normal(rng, shape, jnp.float32) * scale * gain
    return jnp.minimum(jnp.maximum(drawn, -most), most).astype(kind)


def setup_inputs(seed: int = 0) -> dict:
    splits = jax.random.split(jax.random.key(seed), 9)
    sources = gaussian(splits[0], (PX, PY, 2, K, COLS), 1.0, 6.0, ((0, 32), (1, 16)))
    translate_re = gaussian(splits[1], (LEVELS, 2, 2, K, K), (4 * K) ** -0.5, 0.375)
    translate_im = gaussian(splits[2], (LEVELS, 2, 2, K, K), (4 * K) ** -0.5, 0.375)
    frame_index = plant(jax.random.randint(splits[3], (PX, PY, FRAMES), 0, VGRID), jax.random.fold_in(splits[3], 1), 0, VGRID - 1).astype(jnp.int32)
    velocity_index = plant(jax.random.randint(splits[4], (PX, PY, VEL_DEV), 0, VGRID), jax.random.fold_in(splits[4], 1), 0, VGRID - 1).astype(jnp.int32)
    eval_re = gaussian(splits[5], (TILE * TILE, K), (K // 4) ** -0.5, 1.5)
    eval_im = gaussian(splits[6], (TILE * TILE, K), (K // 4) ** -0.5, 1.5)
    window = plant(jax.random.randint(splits[7], (PX, PY), 1, 3), jax.random.fold_in(splits[7], 1), 1, 2).astype(jnp.int32)
    return dict(sources=sources, translate_re=translate_re, translate_im=translate_im, frame_index=frame_index, velocity_index=velocity_index, eval_re=eval_re, eval_im=eval_im, window=window)


TWO_PI = 2.0 * math.pi


def blocks(real_part, imag_part):
    upper = jnp.concatenate([real_part, -imag_part], axis=-1)
    lower = jnp.concatenate([imag_part, real_part], axis=-1)
    return jnp.concatenate([upper, lower], axis=-2)


def angles_of(frame_index, velocity_index, level_no):
    product = (frame_index[..., :, None] * velocity_index[..., None, :] * (level_no + 1)) % VGRID
    angles = (TWO_PI / VGRID) * product.astype(jnp.float32)
    return angles.reshape(angles.shape[:-2] + (COLS,))


def partner_of(state, axis_no, bit_pos):
    shape = state.shape
    count = shape[axis_no]
    stride = 2 ** bit_pos
    split_shape = shape[:axis_no] + (count // (2 * stride), 2, stride) + shape[axis_no + 1:]
    return jnp.flip(state.reshape(split_shape), axis=axis_no + 1).reshape(shape)


def reference(sources, translate_re, translate_im, frame_index, velocity_index, eval_re, eval_im, window):
    state = sources
    row_ids = jnp.arange(N_SX, dtype=jnp.int32)[:, None]
    col_ids = jnp.arange(N_SY, dtype=jnp.int32)[None, :]
    for level_no in range(LEVELS):
        axis_no = level_no % 2
        extent = N_SX if axis_no == 0 else N_SY
        bit_pos = int(extent).bit_length() - 2 - level_no // 2
        partner = partner_of(state, axis_no, bit_pos)
        device_ids = row_ids if axis_no == 0 else col_ids
        bits = jnp.broadcast_to((device_ids >> bit_pos) & 1, (N_SX, N_SY)).astype(jnp.int32)
        angles = angles_of(frame_index, velocity_index, level_no)
        cosine = jnp.cos(angles)
        sine_part = jnp.sin(angles)
        mats_self = blocks(translate_re[level_no][:, 0], translate_im[level_no][:, 0])
        mats_other = blocks(translate_re[level_no][:, 1], translate_im[level_no][:, 1])

        def advance(items):
            own_rows, other_rows, bit_row, cos_row, sin_row = items
            self_pick = mats_self[bit_row].astype(jnp.float32)
            other_pick = mats_other[bit_row].astype(jnp.float32)
            own_flat = own_rows.reshape(N_SY, 2 * K, COLS).astype(jnp.float32)
            other_flat = other_rows.reshape(N_SY, 2 * K, COLS).astype(jnp.float32)
            total = jnp.einsum('dij,djc->dic', self_pick, own_flat) + jnp.einsum('dij,djc->dic', other_pick, other_flat)
            real_total = total[:, :K]
            imag_total = total[:, K:]
            new_real = cos_row[:, None, :] * real_total - sin_row[:, None, :] * imag_total
            new_imag = sin_row[:, None, :] * real_total + cos_row[:, None, :] * imag_total
            return jnp.stack([new_real, new_imag], axis=1).astype(jnp.bfloat16)

        state = lax.map(advance, (state, partner, bits, cosine, sine_part))
    evaluate = jnp.concatenate([eval_re, -eval_im], axis=1).astype(jnp.float32)

    def render(state_row):
        flat_rows = state_row.reshape(N_SY, 2 * K, COLS).astype(jnp.float32)
        tiles = jnp.einsum('pk,ykc->ypc', evaluate, flat_rows).astype(jnp.bfloat16)
        return tiles.reshape(N_SY, TILE, TILE, COLS)

    tiles_all = lax.map(render, state)
    picture = jnp.transpose(tiles_all, (0, 2, 1, 3, 4)).reshape(TX, TY, COLS)
    padded = jnp.pad(picture, ((2, 2), (2, 2), (0, 0)))

    def smooth(row_id):
        values = lax.dynamic_slice_in_dim(padded, row_id * TILE, TILE + 4, 0).astype(jnp.float32)
        rows_near = values[1:-3] + values[2:-2] + values[3:-1]
        rows_far = rows_near + values[0:-4] + values[4:]
        box_near = rows_near[:, 1:-3] + rows_near[:, 2:-2] + rows_near[:, 3:-1]
        box_far = rows_far[:, 1:-3] + rows_far[:, 2:-2] + rows_far[:, 3:-1] + rows_far[:, 0:-4] + rows_far[:, 4:]
        widths = jnp.repeat(window[row_id], TILE)
        chosen = jnp.where(widths[None, :, None] == 2, box_far / 25.0, box_near / 9.0)
        return chosen.astype(jnp.bfloat16)

    smoothed = lax.map(smooth, jnp.arange(N_SX, dtype=jnp.int32))
    return smoothed.reshape(TX, TY, COLS)
```

```python
import functools
import math

import jax
import jax.numpy as jnp
import numpy as np
from jax import lax
from jax.experimental import pallas as pl
from jax.experimental.pallas import tpu as pltpu
from jax.sharding import Mesh
from jax.sharding import PartitionSpec as P

LEVELS = 4
VGRID = 4096
K = 64
TILE = 8
COLS = 4096
BOXES = 64
ZBOX = 8
YBOX = 8
HALF = 64
LANES = 128
WIDE = YBOX * HALF
ROWS = K + 8
TWO_PI = 2.0 * math.pi
GROUP = ("zh", "zl", "y")


def turn(x):
    return jnp.concatenate([x[..., HALF:], x[..., :HALF]], axis=-1)


def lane_low(shape):
    return lax.broadcasted_iota(jnp.int32, shape, len(shape) - 1) % LANES < HALF


def pack_kernel(info_ref, window_ref, frame_ref, velocity_ref, source_ref, out_ref):
    step = pl.program_id(0)
    low = lane_low((K, LANES))
    small_low = lane_low((8, LANES))
    own_row = lax.broadcasted_iota(jnp.int32, (8, LANES), 0) == info_ref[0]
    width = window_ref[0].astype(jnp.float32)
    tiles = source_ref.shape[-1] // LANES
    for tile in range(tiles):
        lanes = pl.ds(tile * LANES, LANES)
        real = source_ref[0, :, lanes].astype(jnp.float32)
        imag = source_ref[1, :, lanes].astype(jnp.float32)
        out_ref[2 * tile, :K, :] = jnp.where(low, real, turn(imag)).astype(jnp.bfloat16)
        out_ref[2 * tile + 1, :K, :] = jnp.where(low, turn(real), imag).astype(jnp.bfloat16)
        frame = frame_ref[step * (tiles // 2) + tile // 2]
        velocity = velocity_ref[:, pl.ds((tile % 2) * LANES, LANES)]
        product = jnp.broadcast_to((frame * velocity) & (VGRID - 1), (8, LANES))
        high_part = (product >> 6).astype(jnp.float32)
        low_part = (product & 63).astype(jnp.float32)
        even = jnp.where(small_low, high_part, turn(low_part))
        odd = jnp.where(small_low, turn(high_part), low_part)
        out_ref[2 * tile, K:, :] = jnp.where(own_row, even, width).astype(jnp.bfloat16)
        out_ref[2 * tile + 1, K:, :] = jnp.where(own_row, odd, width).astype(jnp.bfloat16)


def pack(info, window, frame_index, velocity_index, sources):
    steps = 4
    width = COLS // steps
    return pl.pallas_call(
        pack_kernel,
        grid=(steps,),
        out_shape=jax.ShapeDtypeStruct((BOXES, ROWS, LANES), jnp.bfloat16),
        in_specs=[
            pl.BlockSpec(memory_space=pltpu.SMEM),
            pl.BlockSpec(memory_space=pltpu.SMEM),
            pl.BlockSpec(memory_space=pltpu.SMEM),
            pl.BlockSpec((1, 2 * LANES), lambda s: (0, 0)),
            pl.BlockSpec((2, K, width), lambda s: (0, 0, s)),
        ],
        out_specs=pl.BlockSpec((BOXES // steps, ROWS, LANES), lambda s: (s, 0, 0)),
        cost_estimate=pl.CostEstimate(flops=4 << 20, bytes_accessed=2 << 20, transcendentals=0),
        name="pack",
    )(info, window, frame_index, velocity_index, sources)


def butterfly_kernel(
    info_ref,
    got_ref,
    mats_ref,
    eval_ref,
    picture_ref,
    below_ref,
    above_ref,
    width_ref,
    state_ref,
    cos_ref,
    sin_ref,
):
    low = lane_low((K, LANES))
    small_low = lane_low((8, LANES))
    row = lax.broadcasted_iota(jnp.int32, (8, LANES), 0)
    for pair in range(YBOX // 2):
        lanes = pl.ds(pair * LANES, LANES)
        indices = []
        widths = []
        for y in (2 * pair, 2 * pair + 1):
            index = jnp.zeros((8, LANES), jnp.float32)
            width = jnp.zeros((8, LANES), jnp.float32)
            for z in range(ZBOX):
                extra = got_ref[z * YBOX + y, K:, :].astype(jnp.float32)
                index = jnp.where(row == z, extra, index)
                width = jnp.where(row == (z + 1) % ZBOX, extra, width)
            indices.append(index)
            widths.append(width)
        high_part = jnp.where(small_low, indices[0], turn(indices[1]))
        low_part = jnp.where(small_low, turn(indices[0]), indices[1])
        width_ref[:, lanes] = jnp.where(small_low, widths[0], widths[1])
        angle = (TWO_PI / VGRID) * (64.0 * high_part + low_part)
        cosine = jnp.cos(angle)
        sine = jnp.sin(angle)
        cos_now, sin_now = cosine, sine
        for level in range(LEVELS):
            cos_ref[level, :, lanes] = cos_now
            sin_ref[level, :, lanes] = sin_now
            if level + 1 < LEVELS:
                cos_now, sin_now = (
                    cos_now * cosine - sin_now * sine,
                    sin_now * cosine + cos_now * sine,
                )
    for z in range(ZBOX):
        for pair in range(YBOX // 2):
            lanes = pl.ds(pair * LANES, LANES)
            even = got_ref[z * YBOX + 2 * pair, :K, :].astype(jnp.float32)
            odd = got_ref[z * YBOX + 2 * pair + 1, :K, :].astype(jnp.float32)
            state_ref[z, :K, lanes] = jnp.where(low, even, turn(odd)).astype(jnp.bfloat16)
            state_ref[z, K:, lanes] = jnp.where(low, turn(even), odd).astype(jnp.bfloat16)

    def rotated(level, z, lanes, total):
        cosine = cos_ref[level, pl.ds(z, 1), lanes]
        sine = sin_ref[level, pl.ds(z, 1), lanes]
        real, imag = total[:K], total[K:]
        state_ref[z, :K, lanes] = (cosine * real - sine * imag).astype(jnp.bfloat16)
        state_ref[z, K:, lanes] = (sine * real + cosine * imag).astype(jnp.bfloat16)

    for level, bit in ((0, 4), (1, 1), (2, 2)):
        for z in range(ZBOX):
            if z & bit:
                continue
            for part in range(2):
                lanes = pl.ds(part * 256, 256)
                both = jnp.concatenate([state_ref[z, :, lanes], state_ref[z | bit, :, lanes]], 0)
                total = jnp.dot(mats_ref[level], both, preferred_element_type=jnp.float32)
                rotated(level, z, lanes, total[: 2 * K])
                rotated(level, z | bit, lanes, total[2 * K :])
    for z in range(ZBOX):
        first, second = pl.ds(0, 256), pl.ds(256, 256)
        both = jnp.concatenate([state_ref[z, :, first], state_ref[z, :, second]], 0)
        total = jnp.dot(mats_ref[3], both, preferred_element_type=jnp.float32)
        rotated(3, z, first, total[: 2 * K])
        rotated(3, z, second, total[2 * K :])
    for z in range(ZBOX):
        picture_ref[z] = jnp.dot(
            eval_ref[...], state_ref[z], preferred_element_type=jnp.float32
        ).astype(jnp.bfloat16)
    last = info_ref[1] == 7
    first = info_ref[1] == 0
    nothing = jnp.zeros((16, WIDE), jnp.bfloat16)
    for z in range(ZBOX):

        @pl.when(last)
        def _():
            below_ref[z] = picture_ref[z - 2, 48:, :] if z >= 2 else nothing

        @pl.when(jnp.logical_not(last))
        def _():
            below_ref[z] = picture_ref[z, 48:, :]

        @pl.when(first)
        def _():
            above_ref[z] = picture_ref[z + 2, :16, :] if z + 2 < ZBOX else nothing

        @pl.when(jnp.logical_not(first))
        def _():
            above_ref[z] = picture_ref[z, :16, :]


def butterfly(info, got, mats, evaluate):
    whole = pl.BlockSpec(memory_space=pltpu.VMEM)
    return pl.pallas_call(
        butterfly_kernel,
        out_shape=(
            jax.ShapeDtypeStruct((ZBOX, K, WIDE), jnp.bfloat16),
            jax.ShapeDtypeStruct((ZBOX, 16, WIDE), jnp.bfloat16),
            jax.ShapeDtypeStruct((ZBOX, 16, WIDE), jnp.bfloat16),
            jax.ShapeDtypeStruct((ZBOX, WIDE), jnp.float32),
        ),
        in_specs=[pl.BlockSpec(memory_space=pltpu.SMEM), whole, whole, whole],
        out_specs=(whole, whole, whole, whole),
        scratch_shapes=[
            pltpu.VMEM((ZBOX, 2 * K, WIDE), jnp.bfloat16),
            pltpu.VMEM((LEVELS, ZBOX, WIDE), jnp.float32),
            pltpu.VMEM((LEVELS, ZBOX, WIDE), jnp.float32),
        ],
        cost_estimate=pl.CostEstimate(flops=2 << 30, bytes_accessed=3 << 20, transcendentals=8192),
        name="butterfly",
    )(info, got, mats, evaluate)


def smooth_kernel(picture_ref, below_ref, above_ref, width_ref, sums_ref, out_ref):
    rows = K + 32
    low = lane_low((rows, LANES))
    half_low = lane_low((32, LANES))
    upper = lax.broadcasted_iota(jnp.int32, (rows, LANES), 0) % 8 >= 4
    nothing = jnp.zeros((rows, LANES), jnp.float32)

    def tile(z, pair):
        lanes = pl.ds(pair * LANES, LANES)
        parts = [below_ref[z, :, lanes], picture_ref[z, :, lanes], above_ref[z, :, lanes]]
        return jnp.concatenate(parts, axis=0).astype(jnp.float32)

    for zh in range(ZBOX // 2):
        line = [(2 * zh + i // 4, i % 4) for i in range(8)]
        before, here = nothing, tile(*line[0])
        for i, (z, pair) in enumerate(line):
            after = tile(*line[i + 1]) if i + 1 < len(line) else nothing
            left = jnp.where(low, here, before)
            right = jnp.where(low, after, here)
            beside = turn(jnp.where(upper, left, right))
            field = jnp.concatenate([here, beside], axis=0).astype(jnp.bfloat16)
            sums = jnp.dot(sums_ref[...], field, preferred_element_type=jnp.float32)
            wide = width_ref[pl.ds((z + 1) % ZBOX, 1), pl.ds(pair * LANES, LANES)] > 1.5
            chosen = jnp.where(wide, sums[K:] / 25.0, sums[:K] / 9.0)
            top, bottom = chosen[:32], chosen[32:]
            box = z * YBOX + 2 * pair
            out_ref[box] = jnp.where(half_low, top, turn(bottom)).astype(jnp.bfloat16)
            out_ref[box + 1] = jnp.where(half_low, turn(top), bottom).astype(jnp.bfloat16)
            before, here = here, after


def smooth(picture, below, above, widths, sums):
    whole = pl.BlockSpec(memory_space=pltpu.VMEM)
    return pl.pallas_call(
        smooth_kernel,
        out_shape=jax.ShapeDtypeStruct((BOXES, 32, LANES), jnp.bfloat16),
        in_specs=[whole] * 5,
        out_specs=whole,
        cost_estimate=pl.CostEstimate(flops=1 << 28, bytes_accessed=2 << 20, transcendentals=0),
        name="smooth",
    )(picture, below, above, widths, sums)


def unpack_kernel(got_ref, out_ref):
    low = lane_low((32, LANES))
    for tile in range(out_ref.shape[-1] // LANES):
        lanes = pl.ds(tile * LANES, LANES)
        even = got_ref[2 * tile].astype(jnp.float32)
        odd = got_ref[2 * tile + 1].astype(jnp.float32)
        out_ref[:32, lanes] = jnp.where(low, even, turn(odd)).astype(jnp.bfloat16)
        out_ref[32:, lanes] = jnp.where(low, turn(even), odd).astype(jnp.bfloat16)


def unpack(got):
    steps = 2
    return pl.pallas_call(
        unpack_kernel,
        grid=(steps,),
        out_shape=jax.ShapeDtypeStruct((K, COLS), jnp.bfloat16),
        in_specs=[pl.BlockSpec((BOXES // steps, 32, LANES), lambda s: (s, 0, 0))],
        out_specs=pl.BlockSpec((K, COLS // steps), lambda s: (0, s)),
        cost_estimate=pl.CostEstimate(flops=1 << 20, bytes_accessed=1 << 20, transcendentals=0),
        name="unpack",
    )(got)


def box_sums():
    sums = np.zeros((2, TILE, TILE, 2, TILE + 4, TILE), np.float32)
    for reach in (1, 2):
        for a in range(TILE):
            for b in range(TILE):
                for x in range(TILE + 4):
                    for y in range(TILE):
                        if abs(x - 2 - a) > reach:
                            continue
                        other = y - TILE if y >= 4 else y + TILE
                        sums[reach - 1, a, b, 0, x, y] = abs(y - b) <= reach
                        sums[reach - 1, a, b, 1, x, y] = abs(other - b) <= reach
    return sums.reshape(2 * K, 2 * (K + 32))


def blocks(real_part, imag_part):
    upper = jnp.concatenate([real_part, -imag_part], axis=-1)
    lower = jnp.concatenate([imag_part, real_part], axis=-1)
    return jnp.concatenate([upper, lower], axis=-2)


def on_device(
    sources, translate_re, translate_im, frame_index, velocity_index, eval_re, eval_im, window
):
    z = lax.axis_index("zh") * 2 + lax.axis_index("zl")
    place = lax.broadcasted_iota(jnp.int32, (2,), 0)
    info = jnp.where(place == 0, z, lax.axis_index("xc"))
    message = pack(
        info, window.reshape(1), frame_index.reshape(16), velocity_index.reshape(1, 256), sources[0, 0]
    )
    got = lax.all_to_all(message, GROUP, 0, 0, tiled=True)
    own = blocks(translate_re[:, :, 0], translate_im[:, :, 0])
    other = blocks(translate_re[:, :, 1], translate_im[:, :, 1])
    mats = jnp.concatenate(
        [
            jnp.concatenate([own[:, 0], other[:, 0]], axis=-1),
            jnp.concatenate([other[:, 1], own[:, 1]], axis=-1),
        ],
        axis=-2,
    )
    evaluate = jnp.concatenate([eval_re, -eval_im], axis=1)
    picture, last_rows, first_rows, widths = butterfly(info, got, mats, evaluate)
    below = lax.ppermute(last_rows, "xc", [(i, (i + 1) % 8) for i in range(8)])
    above = lax.ppermute(first_rows, "xc", [(i, (i + 7) % 8) for i in range(8)])
    smoothed = smooth(picture, below, above, widths, jnp.asarray(box_sums(), jnp.bfloat16))
    back = lax.all_to_all(smoothed, GROUP, 0, 0, tiled=True)
    return unpack(back).reshape(TILE, TILE, COLS)


def solution(mesh):
    fine = Mesh(mesh.devices.reshape(4, 8, 2, 8), ("zh", "xc", "zl", "y"))
    box = (("zh", "xc"), ("zl", "y"))
    return jax.shard_map(
        on_device,
        mesh=fine,
        in_specs=(
            P(*box, None, None, None),
            P(),
            P(),
            P(*box, None),
            P(*box, None),
            P(),
            P(),
            P(*box),
        ),
        out_specs=P(*box, None),
        check_vma=False,
    )
```

```python
import functools
import math

import jax
import jax.numpy as jnp
import numpy as np
from jax import lax
from jax.experimental import pallas as pl
from jax.experimental.pallas import tpu as pltpu
from jax.sharding import Mesh
from jax.sharding import PartitionSpec as P

LEVELS = 4
VGRID = 4096
K = 64
TILE = 8
COLS = 4096
BOXES = 64
ZBOX = 8
YBOX = 8
HALF = 64
LANES = 128
WIDE = YBOX * HALF
ROWS = K + 2
TWO_PI = 2.0 * math.pi
GROUP = ("zh", "zl", "y")


def turn(x):
    return jnp.concatenate([x[..., HALF:], x[..., :HALF]], axis=-1)


def lane_low(shape):
    return lax.broadcasted_iota(jnp.int32, shape, len(shape) - 1) % LANES < HALF


def pack_kernel(window_ref, frame_ref, velocity_ref, source_ref, out_ref):
    step = pl.program_id(0)
    low = lane_low((1, LANES))
    tiles = source_ref.shape[-1] // LANES
    out = out_ref.reshape(2 * tiles, ROWS, LANES)
    width = jnp.full((1, LANES), window_ref[0].astype(jnp.float32))
    for tile in range(tiles):
        lanes = pl.ds(tile * LANES, LANES)
        real = source_ref[0, :, lanes]
        imag = source_ref[1, :, lanes]
        out[2 * tile, :K, :] = jnp.concatenate([real[:, :HALF], imag[:, :HALF]], axis=1)
        out[2 * tile + 1, :K, :] = jnp.concatenate([real[:, HALF:], imag[:, HALF:]], axis=1)
        frame = frame_ref[step * (tiles // 2) + tile // 2]
        velocity = velocity_ref[:, pl.ds((tile % 2) * LANES, LANES)]
        product = (frame * velocity) & (VGRID - 1)
        high_part = (product >> 6).astype(jnp.float32)
        low_part = (product & 63).astype(jnp.float32)
        even = jnp.where(low, high_part, turn(low_part))
        odd = jnp.where(low, turn(high_part), low_part)
        out[2 * tile, K:, :] = jnp.concatenate([even, width], axis=0).astype(jnp.bfloat16)
        out[2 * tile + 1, K:, :] = jnp.concatenate([odd, width], axis=0).astype(jnp.bfloat16)


def pack(window, frame_index, velocity_index, sources):
    steps = 2
    width = COLS // steps
    return pl.pallas_call(
        pack_kernel,
        grid=(steps,),
        out_shape=jax.ShapeDtypeStruct((BOXES, ROWS // 2, 2, LANES), jnp.bfloat16),
        in_specs=[
            pl.BlockSpec(memory_space=pltpu.SMEM),
            pl.BlockSpec(memory_space=pltpu.SMEM),
            pl.BlockSpec((1, 2 * LANES), lambda s: (0, 0)),
            pl.BlockSpec((2, K, width), lambda s: (0, 0, s)),
        ],
        out_specs=pl.BlockSpec((BOXES // steps, ROWS // 2, 2, LANES), lambda s: (s, 0, 0, 0)),
        cost_estimate=pl.CostEstimate(flops=4 << 20, bytes_accessed=2 << 20, transcendentals=0),
        name="pack",
    )(window, frame_index, velocity_index, sources)


def butterfly_kernel(
    place_ref,
    message_ref,
    mats_ref,
    eval_ref,
    picture_ref,
    below_ref,
    above_ref,
    width_ref,
    state_ref,
    cos_ref,
    sin_ref,
):
    got_ref = message_ref.reshape(BOXES, ROWS, LANES)
    small_low = lane_low((8, LANES))
    row = lax.broadcasted_iota(jnp.int32, (8, LANES), 0)
    for pair in range(YBOX // 2):
        lanes = pl.ds(pair * LANES, LANES)
        indices = []
        widths = []
        for y in (2 * pair, 2 * pair + 1):
            index = jnp.zeros((8, LANES), jnp.float32)
            width = jnp.zeros((8, LANES), jnp.float32)
            for z in range(ZBOX):
                extra = got_ref[z * YBOX + y, K:, :].astype(jnp.float32)
                index = jnp.where(row == z, extra[:1], index)
                width = jnp.where(row == z, extra[1:], width)
            indices.append(index)
            widths.append(width)
        high_part = jnp.where(small_low, indices[0], turn(indices[1]))
        low_part = jnp.where(small_low, turn(indices[0]), indices[1])
        width_ref[:, lanes] = jnp.where(small_low, widths[0], widths[1])
        angle = (TWO_PI / VGRID) * (64.0 * high_part + low_part)
        cosine = jnp.cos(angle)
        sine = jnp.sin(angle)
        cos_now, sin_now = cosine, sine
        for level in range(LEVELS):
            cos_ref[level, :, lanes] = cos_now
            sin_ref[level, :, lanes] = sin_now
            if level + 1 < LEVELS:
                cos_now, sin_now = (
                    cos_now * cosine - sin_now * sine,
                    sin_now * cosine + cos_now * sine,
                )
    for z in range(ZBOX):
        for pair in range(YBOX // 2):
            lanes = pl.ds(pair * LANES, LANES)
            even = got_ref[z * YBOX + 2 * pair, :K, :]
            odd = got_ref[z * YBOX + 2 * pair + 1, :K, :]
            state_ref[z, :K, lanes] = jnp.concatenate([even[:, :HALF], odd[:, :HALF]], axis=1)
            state_ref[z, K:, lanes] = jnp.concatenate([even[:, HALF:], odd[:, HALF:]], axis=1)

    def rotated(level, z, lanes, total):
        cosine = cos_ref[level, pl.ds(z, 1), lanes]
        sine = sin_ref[level, pl.ds(z, 1), lanes]
        real, imag = total[:K], total[K:]
        state_ref[z, :K, lanes] = (cosine * real - sine * imag).astype(jnp.bfloat16)
        state_ref[z, K:, lanes] = (sine * real + cosine * imag).astype(jnp.bfloat16)

    for level, bit in ((0, 4), (1, 1), (2, 2)):
        for z in range(ZBOX):
            if z & bit:
                continue
            for part in range(2):
                lanes = pl.ds(part * 256, 256)
                both = jnp.concatenate([state_ref[z, :, lanes], state_ref[z | bit, :, lanes]], 0)
                total = jnp.dot(mats_ref[level], both, preferred_element_type=jnp.float32)
                rotated(level, z, lanes, total[: 2 * K])
                rotated(level, z | bit, lanes, total[2 * K :])
    for z in range(ZBOX):
        first, second = pl.ds(0, 256), pl.ds(256, 256)
        both = jnp.concatenate([state_ref[z, :, first], state_ref[z, :, second]], 0)
        total = jnp.dot(mats_ref[3], both, preferred_element_type=jnp.float32)
        rotated(3, z, first, total[: 2 * K])
        rotated(3, z, second, total[2 * K :])
    for z in range(ZBOX):
        picture_ref[z] = jnp.dot(
            eval_ref[...], state_ref[z], preferred_element_type=jnp.float32
        ).astype(jnp.bfloat16)
    last = place_ref[0] == 7
    first = place_ref[0] == 0
    nothing = jnp.zeros((16, WIDE), jnp.bfloat16)
    for z in range(ZBOX):

        @pl.when(last)
        def _():
            below_ref[z] = picture_ref[z - 2, 48:, :] if z >= 2 else nothing

        @pl.when(jnp.logical_not(last))
        def _():
            below_ref[z] = picture_ref[z, 48:, :]

        @pl.when(first)
        def _():
            above_ref[z] = picture_ref[z + 2, :16, :] if z + 2 < ZBOX else nothing

        @pl.when(jnp.logical_not(first))
        def _():
            above_ref[z] = picture_ref[z, :16, :]


def butterfly(place, got, mats, evaluate):
    whole = pl.BlockSpec(memory_space=pltpu.VMEM)
    return pl.pallas_call(
        butterfly_kernel,
        out_shape=(
            jax.ShapeDtypeStruct((ZBOX, K, WIDE), jnp.bfloat16),
            jax.ShapeDtypeStruct((ZBOX, 16, WIDE), jnp.bfloat16),
            jax.ShapeDtypeStruct((ZBOX, 16, WIDE), jnp.bfloat16),
            jax.ShapeDtypeStruct((ZBOX, WIDE), jnp.float32),
        ),
        in_specs=[pl.BlockSpec(memory_space=pltpu.SMEM), whole, whole, whole],
        out_specs=(whole, whole, whole, whole),
        scratch_shapes=[
            pltpu.VMEM((ZBOX, 2 * K, WIDE), jnp.bfloat16),
            pltpu.VMEM((LEVELS, ZBOX, WIDE), jnp.float32),
            pltpu.VMEM((LEVELS, ZBOX, WIDE), jnp.float32),
        ],
        cost_estimate=pl.CostEstimate(flops=2 << 30, bytes_accessed=3 << 20, transcendentals=8192),
        compiler_params=pltpu.CompilerParams(vmem_limit_bytes=12 << 20),
        name="butterfly",
    )(place, got, mats, evaluate)


def smooth_kernel(picture_ref, below_ref, above_ref, width_ref, sums_ref, out_ref):
    rows = K + 32
    low = lane_low((rows, LANES))
    half_low = lane_low((32, LANES))
    upper = lax.broadcasted_iota(jnp.int32, (rows, LANES), 0) % 8 >= 4
    nothing = jnp.zeros((rows, LANES), jnp.float32)

    def tile(z, pair):
        lanes = pl.ds(pair * LANES, LANES)
        parts = [below_ref[z, :, lanes], picture_ref[z, :, lanes], above_ref[z, :, lanes]]
        return jnp.concatenate(parts, axis=0).astype(jnp.float32)

    for zh in range(ZBOX // 2):
        line = [(2 * zh + i // 4, i % 4) for i in range(8)]
        before, here = nothing, tile(*line[0])
        for i, (z, pair) in enumerate(line):
            after = tile(*line[i + 1]) if i + 1 < len(line) else nothing
            left = jnp.where(low, here, before)
            right = jnp.where(low, after, here)
            beside = turn(jnp.where(upper, left, right))
            field = jnp.concatenate([here, beside], axis=0).astype(jnp.bfloat16)
            sums = jnp.dot(sums_ref[...], field, preferred_element_type=jnp.float32)
            wide = width_ref[pl.ds(z, 1), pl.ds(pair * LANES, LANES)] > 1.5
            chosen = jnp.where(wide, sums[K:] / 25.0, sums[:K] / 9.0)
            top, bottom = chosen[:32], chosen[32:]
            box = z * YBOX + 2 * pair
            out_ref[box] = jnp.where(half_low, top, turn(bottom)).astype(jnp.bfloat16)
            out_ref[box + 1] = jnp.where(half_low, turn(top), bottom).astype(jnp.bfloat16)
            before, here = here, after


def smooth(picture, below, above, widths, sums):
    whole = pl.BlockSpec(memory_space=pltpu.VMEM)
    return pl.pallas_call(
        smooth_kernel,
        out_shape=jax.ShapeDtypeStruct((BOXES, 32, LANES), jnp.bfloat16),
        in_specs=[whole] * 5,
        out_specs=whole,
        cost_estimate=pl.CostEstimate(flops=1 << 28, bytes_accessed=2 << 20, transcendentals=0),
        compiler_params=pltpu.CompilerParams(vmem_limit_bytes=12 << 20),
        name="smooth",
    )(picture, below, above, widths, sums)


def unpack_kernel(got_ref, out_ref):
    for tile in range(out_ref.shape[-1] // LANES):
        lanes = pl.ds(tile * LANES, LANES)
        even = got_ref[2 * tile]
        odd = got_ref[2 * tile + 1]
        out_ref[:32, lanes] = jnp.concatenate([even[:, :HALF], odd[:, :HALF]], axis=1)
        out_ref[32:, lanes] = jnp.concatenate([even[:, HALF:], odd[:, HALF:]], axis=1)


def unpack(got):
    steps = 2
    return pl.pallas_call(
        unpack_kernel,
        grid=(steps,),
        out_shape=jax.ShapeDtypeStruct((K, COLS), jnp.bfloat16),
        in_specs=[pl.BlockSpec((BOXES // steps, 32, LANES), lambda s: (s, 0, 0))],
        out_specs=pl.BlockSpec((K, COLS // steps), lambda s: (0, s)),
        cost_estimate=pl.CostEstimate(flops=1 << 20, bytes_accessed=1 << 20, transcendentals=0),
        compiler_params=pltpu.CompilerParams(vmem_limit_bytes=12 << 20),
        name="unpack",
    )(got)


def box_sums():
    sums = np.zeros((2, TILE, TILE, 2, TILE + 4, TILE), np.float32)
    for reach in (1, 2):
        for a in range(TILE):
            for b in range(TILE):
                for x in range(TILE + 4):
                    for y in range(TILE):
                        if abs(x - 2 - a) > reach:
                            continue
                        other = y - TILE if y >= 4 else y + TILE
                        sums[reach - 1, a, b, 0, x, y] = abs(y - b) <= reach
                        sums[reach - 1, a, b, 1, x, y] = abs(other - b) <= reach
    return sums.reshape(2 * K, 2 * (K + 32))


def blocks(real_part, imag_part):
    upper = jnp.concatenate([real_part, -imag_part], axis=-1)
    lower = jnp.concatenate([imag_part, real_part], axis=-1)
    return jnp.concatenate([upper, lower], axis=-2)


def on_device(
    sources, translate_re, translate_im, frame_index, velocity_index, eval_re, eval_im, window
):
    message = pack(
        window.reshape(1), frame_index.reshape(16), velocity_index.reshape(1, 256), sources[0, 0]
    )
    got = lax.all_to_all(message, GROUP, 0, 0, tiled=True)
    own = blocks(translate_re[:, :, 0], translate_im[:, :, 0])
    other = blocks(translate_re[:, :, 1], translate_im[:, :, 1])
    mats = jnp.concatenate(
        [
            jnp.concatenate([own[:, 0], other[:, 0]], axis=-1),
            jnp.concatenate([other[:, 1], own[:, 1]], axis=-1),
        ],
        axis=-2,
    )
    evaluate = jnp.concatenate([eval_re, -eval_im], axis=1)
    picture, last_rows, first_rows, widths = butterfly(lax.axis_index("xc").reshape(1), got, mats, evaluate)
    below = lax.ppermute(last_rows, "xc", [(i, (i + 1) % 8) for i in range(8)])
    above = lax.ppermute(first_rows, "xc", [(i, (i + 7) % 8) for i in range(8)])
    smoothed = smooth(picture, below, above, widths, jnp.asarray(box_sums(), jnp.bfloat16))
    back = lax.all_to_all(smoothed, GROUP, 0, 0, tiled=True)
    return unpack(back).reshape(TILE, TILE, COLS)


def solution(mesh):
    fine = Mesh(mesh.devices.reshape(4, 8, 2, 8), ("zh", "xc", "zl", "y"))
    box = (("zh", "xc"), ("zl", "y"))
    return jax.shard_map(
        on_device,
        mesh=fine,
        in_specs=(
            P(*box, None, None, None),
            P(),
            P(),
            P(*box, None),
            P(*box, None),
            P(),
            P(),
            P(*box),
        ),
        out_specs=P(*box, None),
        check_vma=False,
    )
```

```python
import functools
import math

import jax
import jax.numpy as jnp
import numpy as np
from jax import lax
from jax.experimental import pallas as pl
from jax.experimental.pallas import tpu as pltpu
from jax.sharding import Mesh
from jax.sharding import PartitionSpec as P

LEVELS = 4
VGRID = 4096
K = 64
TILE = 8
COLS = 4096
BOXES = 64
ZBOX = 8
YBOX = 8
HALF = 64
LANES = 128
WIDE = YBOX * HALF
ROWS = K + 2
TWO_PI = 2.0 * math.pi
GROUP = ("zh", "zl", "y")


def turn(x):
    return jnp.concatenate([x[..., HALF:], x[..., :HALF]], axis=-1)


def lane_low(shape):
    return lax.broadcasted_iota(jnp.int32, shape, len(shape) - 1) % LANES < HALF


def pack_kernel(window_ref, frame_ref, velocity_ref, source_ref, out_ref):
    step = pl.program_id(0)
    low = lane_low((1, LANES))
    tiles = source_ref.shape[-1] // LANES
    out = out_ref.reshape(2 * tiles, ROWS, LANES)
    width = jnp.full((1, LANES), window_ref[0].astype(jnp.float32))
    for tile in range(tiles):
        lanes = pl.ds(tile * LANES, LANES)
        real = source_ref[0, :, lanes]
        imag = source_ref[1, :, lanes]
        out[2 * tile, :K, :] = jnp.concatenate([real[:, :HALF], imag[:, :HALF]], axis=1)
        out[2 * tile + 1, :K, :] = jnp.concatenate([real[:, HALF:], imag[:, HALF:]], axis=1)
        frame = frame_ref[step * (tiles // 2) + tile // 2]
        velocity = velocity_ref[:, pl.ds((tile % 2) * LANES, LANES)]
        product = (frame * velocity) & (VGRID - 1)
        high_part = (product >> 6).astype(jnp.float32)
        low_part = (product & 63).astype(jnp.float32)
        even = jnp.where(low, high_part, turn(low_part))
        odd = jnp.where(low, turn(high_part), low_part)
        out[2 * tile, K:, :] = jnp.concatenate([even, width], axis=0).astype(jnp.bfloat16)
        out[2 * tile + 1, K:, :] = jnp.concatenate([odd, width], axis=0).astype(jnp.bfloat16)


def pack(window, frame_index, velocity_index, sources):
    steps = 2
    width = COLS // steps
    return pl.pallas_call(
        pack_kernel,
        grid=(steps,),
        out_shape=jax.ShapeDtypeStruct((BOXES, ROWS // 2, 2, LANES), jnp.bfloat16),
        in_specs=[
            pl.BlockSpec(memory_space=pltpu.SMEM),
            pl.BlockSpec(memory_space=pltpu.SMEM),
            pl.BlockSpec((1, 2 * LANES), lambda s: (0, 0)),
            pl.BlockSpec((2, K, width), lambda s: (0, 0, s)),
        ],
        out_specs=pl.BlockSpec((BOXES // steps, ROWS // 2, 2, LANES), lambda s: (s, 0, 0, 0)),
        cost_estimate=pl.CostEstimate(flops=4 << 20, bytes_accessed=2 << 20, transcendentals=0),
        name="pack",
    )(window, frame_index, velocity_index, sources)


def butterfly_kernel(
    place_ref,
    message_ref,
    mats_ref,
    eval_ref,
    picture_ref,
    inner_ref,
    outer_ref,
    width_ref,
    state_ref,
    cos_ref,
    sin_ref,
):
    got_ref = message_ref.reshape(BOXES, ROWS, LANES)
    small_low = lane_low((8, LANES))
    row = lax.broadcasted_iota(jnp.int32, (8, LANES), 0)
    for pair in range(YBOX // 2):
        lanes = pl.ds(pair * LANES, LANES)
        indices = []
        widths = []
        for y in (2 * pair, 2 * pair + 1):
            index = jnp.zeros((8, LANES), jnp.float32)
            width = jnp.zeros((8, LANES), jnp.float32)
            for z in range(ZBOX):
                extra = got_ref[z * YBOX + y, K:, :].astype(jnp.float32)
                index = jnp.where(row == z, extra[:1], index)
                width = jnp.where(row == z, extra[1:], width)
            indices.append(index)
            widths.append(width)
        high_part = jnp.where(small_low, indices[0], turn(indices[1]))
        low_part = jnp.where(small_low, turn(indices[0]), indices[1])
        width_ref[:, lanes] = jnp.where(small_low, widths[0], widths[1])
        angle = (TWO_PI / VGRID) * (64.0 * high_part + low_part)
        cosine = jnp.cos(angle)
        sine = jnp.sin(angle)
        cos_now, sin_now = cosine, sine
        for level in range(LEVELS):
            cos_ref[level, :, lanes] = cos_now
            sin_ref[level, :, lanes] = sin_now
            if level + 1 < LEVELS:
                cos_now, sin_now = (
                    cos_now * cosine - sin_now * sine,
                    sin_now * cosine + cos_now * sine,
                )
    for z in range(ZBOX):
        for pair in range(YBOX // 2):
            lanes = pl.ds(pair * LANES, LANES)
            even = got_ref[z * YBOX + 2 * pair, :K, :]
            odd = got_ref[z * YBOX + 2 * pair + 1, :K, :]
            state_ref[z, :K, lanes] = jnp.concatenate([even[:, :HALF], odd[:, :HALF]], axis=1)
            state_ref[z, K:, lanes] = jnp.concatenate([even[:, HALF:], odd[:, HALF:]], axis=1)

    def rotated(level, z, lanes, total):
        cosine = cos_ref[level, pl.ds(z, 1), lanes]
        sine = sin_ref[level, pl.ds(z, 1), lanes]
        real, imag = total[:K], total[K:]
        state_ref[z, :K, lanes] = (cosine * real - sine * imag).astype(jnp.bfloat16)
        state_ref[z, K:, lanes] = (sine * real + cosine * imag).astype(jnp.bfloat16)

    for level, bit in ((0, 4), (1, 1), (2, 2)):
        for z in range(ZBOX):
            if z & bit:
                continue
            for part in range(2):
                lanes = pl.ds(part * 256, 256)
                both = jnp.concatenate([state_ref[z, :, lanes], state_ref[z | bit, :, lanes]], 0)
                total = jnp.dot(mats_ref[level], both, preferred_element_type=jnp.float32)
                rotated(level, z, lanes, total[: 2 * K])
                rotated(level, z | bit, lanes, total[2 * K :])
    for z in range(ZBOX):
        first, second = pl.ds(0, 256), pl.ds(256, 256)
        both = jnp.concatenate([state_ref[z, :, first], state_ref[z, :, second]], 0)
        total = jnp.dot(mats_ref[3], both, preferred_element_type=jnp.float32)
        rotated(3, z, first, total[: 2 * K])
        rotated(3, z, second, total[2 * K :])
    for z in range(ZBOX):
        picture_ref[z] = jnp.dot(
            eval_ref[...], state_ref[z], preferred_element_type=jnp.float32
        ).astype(jnp.bfloat16)
    place = place_ref[0]
    even = place % 2 == 0
    for z in range(ZBOX):
        first_rows, last_rows = picture_ref[z, :16, :], picture_ref[z, 48:, :]
        nothing = jnp.zeros_like(first_rows)
        next_rows = picture_ref[z + 2, :16, :] if z + 2 < ZBOX else nothing
        previous_rows = picture_ref[z - 2, 48:, :] if z >= 2 else nothing

        @pl.when(even)
        def _():
            inner_ref[z] = last_rows
            outer_ref[z] = jnp.where(place == 0, next_rows, first_rows)

        @pl.when(jnp.logical_not(even))
        def _():
            inner_ref[z] = first_rows
            outer_ref[z] = jnp.where(place == 7, previous_rows, last_rows)


def butterfly(place, got, mats, evaluate):
    whole = pl.BlockSpec(memory_space=pltpu.VMEM)
    return pl.pallas_call(
        butterfly_kernel,
        out_shape=(
            jax.ShapeDtypeStruct((ZBOX, K, WIDE), jnp.bfloat16),
            jax.ShapeDtypeStruct((ZBOX, 16, WIDE), jnp.bfloat16),
            jax.ShapeDtypeStruct((ZBOX, 16, WIDE), jnp.bfloat16),
            jax.ShapeDtypeStruct((ZBOX, WIDE), jnp.float32),
        ),
        in_specs=[pl.BlockSpec(memory_space=pltpu.SMEM), whole, whole, whole],
        out_specs=(whole, whole, whole, whole),
        scratch_shapes=[
            pltpu.VMEM((ZBOX, 2 * K, WIDE), jnp.bfloat16),
            pltpu.VMEM((LEVELS, ZBOX, WIDE), jnp.float32),
            pltpu.VMEM((LEVELS, ZBOX, WIDE), jnp.float32),
        ],
        cost_estimate=pl.CostEstimate(flops=2 << 30, bytes_accessed=3 << 20, transcendentals=8192),
        compiler_params=pltpu.CompilerParams(vmem_limit_bytes=12 << 20),
        name="butterfly",
    )(place, got, mats, evaluate)


def smooth_kernel(place_ref, picture_ref, inner_ref, outer_ref, width_ref, sums_ref, out_ref):
    rows = K + 32
    even = place_ref[0] % 2 == 0
    low = lane_low((rows, LANES))
    half_low = lane_low((32, LANES))
    upper = lax.broadcasted_iota(jnp.int32, (rows, LANES), 0) % 8 >= 4
    nothing = jnp.zeros((rows, LANES), jnp.float32)

    def tile(z, pair):
        lanes = pl.ds(pair * LANES, LANES)
        inner, outer = inner_ref[z, :, lanes], outer_ref[z, :, lanes]
        below, above = jnp.where(even, outer, inner), jnp.where(even, inner, outer)
        parts = [below, picture_ref[z, :, lanes], above]
        return jnp.concatenate(parts, axis=0).astype(jnp.float32)

    for zh in range(ZBOX // 2):
        line = [(2 * zh + i // 4, i % 4) for i in range(8)]
        before, here = nothing, tile(*line[0])
        for i, (z, pair) in enumerate(line):
            after = tile(*line[i + 1]) if i + 1 < len(line) else nothing
            left = jnp.where(low, here, before)
            right = jnp.where(low, after, here)
            beside = turn(jnp.where(upper, left, right))
            field = jnp.concatenate([here, beside], axis=0).astype(jnp.bfloat16)
            sums = jnp.dot(sums_ref[...], field, preferred_element_type=jnp.float32)
            wide = width_ref[pl.ds(z, 1), pl.ds(pair * LANES, LANES)] > 1.5
            chosen = jnp.where(wide, sums[K:] / 25.0, sums[:K] / 9.0)
            top, bottom = chosen[:32], chosen[32:]
            box = z * YBOX + 2 * pair
            out_ref[box] = jnp.where(half_low, top, turn(bottom)).astype(jnp.bfloat16)
            out_ref[box + 1] = jnp.where(half_low, turn(top), bottom).astype(jnp.bfloat16)
            before, here = here, after


def smooth(place, picture, inner, outer, widths, sums):
    whole = pl.BlockSpec(memory_space=pltpu.VMEM)
    return pl.pallas_call(
        smooth_kernel,
        out_shape=jax.ShapeDtypeStruct((BOXES, 32, LANES), jnp.bfloat16),
        in_specs=[pl.BlockSpec(memory_space=pltpu.SMEM)] + [whole] * 5,
        out_specs=whole,
        cost_estimate=pl.CostEstimate(flops=1 << 28, bytes_accessed=2 << 20, transcendentals=0),
        compiler_params=pltpu.CompilerParams(vmem_limit_bytes=12 << 20),
        name="smooth",
    )(place, picture, inner, outer, widths, sums)


def unpack_kernel(got_ref, out_ref):
    for tile in range(out_ref.shape[-1] // LANES):
        lanes = pl.ds(tile * LANES, LANES)
        even = got_ref[2 * tile]
        odd = got_ref[2 * tile + 1]
        out_ref[:32, lanes] = jnp.concatenate([even[:, :HALF], odd[:, :HALF]], axis=1)
        out_ref[32:, lanes] = jnp.concatenate([even[:, HALF:], odd[:, HALF:]], axis=1)


def unpack(got):
    steps = 2
    return pl.pallas_call(
        unpack_kernel,
        grid=(steps,),
        out_shape=jax.ShapeDtypeStruct((K, COLS), jnp.bfloat16),
        in_specs=[pl.BlockSpec((BOXES // steps, 32, LANES), lambda s: (s, 0, 0))],
        out_specs=pl.BlockSpec((K, COLS // steps), lambda s: (0, s)),
        cost_estimate=pl.CostEstimate(flops=1 << 20, bytes_accessed=1 << 20, transcendentals=0),
        compiler_params=pltpu.CompilerParams(vmem_limit_bytes=12 << 20),
        name="unpack",
    )(got)


def box_sums():
    sums = np.zeros((2, TILE, TILE, 2, TILE + 4, TILE), np.float32)
    for reach in (1, 2):
        for a in range(TILE):
            for b in range(TILE):
                for x in range(TILE + 4):
                    for y in range(TILE):
                        if abs(x - 2 - a) > reach:
                            continue
                        other = y - TILE if y >= 4 else y + TILE
                        sums[reach - 1, a, b, 0, x, y] = abs(y - b) <= reach
                        sums[reach - 1, a, b, 1, x, y] = abs(other - b) <= reach
    return sums.reshape(2 * K, 2 * (K + 32))


def blocks(real_part, imag_part):
    upper = jnp.concatenate([real_part, -imag_part], axis=-1)
    lower = jnp.concatenate([imag_part, real_part], axis=-1)
    return jnp.concatenate([upper, lower], axis=-2)


def on_device(
    sources, translate_re, translate_im, frame_index, velocity_index, eval_re, eval_im, window
):
    message = pack(
        window.reshape(1), frame_index.reshape(16), velocity_index.reshape(1, 256), sources[0, 0]
    )
    got = lax.all_to_all(message, GROUP, 0, 0, tiled=True)
    own = blocks(translate_re[:, :, 0], translate_im[:, :, 0])
    other = blocks(translate_re[:, :, 1], translate_im[:, :, 1])
    mats = jnp.concatenate(
        [
            jnp.concatenate([own[:, 0], other[:, 0]], axis=-1),
            jnp.concatenate([other[:, 1], own[:, 1]], axis=-1),
        ],
        axis=-2,
    )
    evaluate = jnp.concatenate([eval_re, -eval_im], axis=1)
    place = lax.axis_index("xc").reshape(1)
    picture, inner, outer, widths = butterfly(place, got, mats, evaluate)
    inner = lax.ppermute(inner, "xc", [(i, i ^ 1) for i in range(8)])
    outer = lax.ppermute(outer, "xc", [(i, (i + 1 if i % 2 else i + 7) % 8) for i in range(8)])
    sums = jnp.asarray(box_sums(), jnp.bfloat16)
    smoothed = smooth(place, picture, inner, outer, widths, sums)
    back = lax.all_to_all(smoothed, GROUP, 0, 0, tiled=True)
    return unpack(back).reshape(TILE, TILE, COLS)


def solution(mesh):
    fine = Mesh(mesh.devices.reshape(4, 8, 2, 8), ("zh", "xc", "zl", "y"))
    box = (("zh", "xc"), ("zl", "y"))
    return jax.shard_map(
        on_device,
        mesh=fine,
        in_specs=(
            P(*box, None, None, None),
            P(),
            P(),
            P(*box, None),
            P(*box, None),
            P(),
            P(),
            P(*box),
        ),
        out_specs=P(*box, None),
        check_vma=False,
    )
```

```python
import functools
import math

import jax
import jax.numpy as jnp
import numpy as np
from jax import lax
from jax.experimental import pallas as pl
from jax.experimental.pallas import tpu as pltpu
from jax.sharding import Mesh
from jax.sharding import PartitionSpec as P

LEVELS = 4
VGRID = 4096
K = 64
TILE = 8
COLS = 4096
BOXES = 64
ZBOX = 8
YBOX = 8
HALF = 64
LANES = 128
WIDE = YBOX * HALF
ROWS = K + 2
TWO_PI = 2.0 * math.pi
GROUP = ("zh", "zl", "y")


def turn(x):
    return jnp.concatenate([x[..., HALF:], x[..., :HALF]], axis=-1)


def lane_low(shape):
    return lax.broadcasted_iota(jnp.int32, shape, len(shape) - 1) % LANES < HALF


def pack_kernel(window_ref, frame_ref, velocity_ref, source_ref, out_ref):
    step = pl.program_id(0)
    low = lane_low((1, LANES))
    tiles = source_ref.shape[-1] // LANES
    out = out_ref.reshape(2 * tiles, ROWS, LANES)
    width = jnp.full((1, LANES), window_ref[0].astype(jnp.float32))
    for tile in range(tiles):
        lanes = pl.ds(tile * LANES, LANES)
        real = source_ref[0, :, lanes]
        imag = source_ref[1, :, lanes]
        out[2 * tile, :K, :] = jnp.concatenate([real[:, :HALF], imag[:, :HALF]], axis=1)
        out[2 * tile + 1, :K, :] = jnp.concatenate([real[:, HALF:], imag[:, HALF:]], axis=1)
        frame = frame_ref[step * (tiles // 2) + tile // 2]
        velocity = velocity_ref[:, pl.ds((tile % 2) * LANES, LANES)]
        product = (frame * velocity) & (VGRID - 1)
        high_part = (product >> 6).astype(jnp.float32)
        low_part = (product & 63).astype(jnp.float32)
        even = jnp.where(low, high_part, turn(low_part))
        odd = jnp.where(low, turn(high_part), low_part)
        out[2 * tile, K:, :] = jnp.concatenate([even, width], axis=0).astype(jnp.bfloat16)
        out[2 * tile + 1, K:, :] = jnp.concatenate([odd, width], axis=0).astype(jnp.bfloat16)


def pack(window, frame_index, velocity_index, sources):
    steps = 1
    width = COLS // steps
    return pl.pallas_call(
        pack_kernel,
        grid=(steps,),
        out_shape=jax.ShapeDtypeStruct((BOXES, ROWS // 2, 2, LANES), jnp.bfloat16),
        in_specs=[
            pl.BlockSpec(memory_space=pltpu.SMEM),
            pl.BlockSpec(memory_space=pltpu.SMEM),
            pl.BlockSpec((1, 2 * LANES), lambda s: (0, 0)),
            pl.BlockSpec((2, K, width), lambda s: (0, 0, s)),
        ],
        out_specs=pl.BlockSpec((BOXES // steps, ROWS // 2, 2, LANES), lambda s: (s, 0, 0, 0)),
        cost_estimate=pl.CostEstimate(flops=4 << 20, bytes_accessed=2 << 20, transcendentals=0),
        name="pack",
    )(window, frame_index, velocity_index, sources)


def butterfly_kernel(
    place_ref,
    message_ref,
    mats_ref,
    eval_ref,
    picture_ref,
    below_ref,
    above_ref,
    width_ref,
    state_ref,
    cos_ref,
    sin_ref,
):
    got_ref = message_ref.reshape(BOXES, ROWS, LANES)
    small_low = lane_low((8, LANES))
    row = lax.broadcasted_iota(jnp.int32, (8, LANES), 0)
    for pair in range(YBOX // 2):
        lanes = pl.ds(pair * LANES, LANES)
        indices = []
        widths = []
        for y in (2 * pair, 2 * pair + 1):
            index = jnp.zeros((8, LANES), jnp.float32)
            width = jnp.zeros((8, LANES), jnp.float32)
            for z in range(ZBOX):
                extra = got_ref[z * YBOX + y, K:, :].astype(jnp.float32)
                index = jnp.where(row == z, extra[:1], index)
                width = jnp.where(row == z, extra[1:], width)
            indices.append(index)
            widths.append(width)
        high_part = jnp.where(small_low, indices[0], turn(indices[1]))
        low_part = jnp.where(small_low, turn(indices[0]), indices[1])
        width_ref[:, lanes] = jnp.where(small_low, widths[0], widths[1])
        angle = (TWO_PI / VGRID) * (64.0 * high_part + low_part)
        cosine = jnp.cos(angle)
        sine = jnp.sin(angle)
        cos_now, sin_now = cosine, sine
        for level in range(LEVELS):
            cos_ref[level, :, lanes] = cos_now
            sin_ref[level, :, lanes] = sin_now
            if level + 1 < LEVELS:
                cos_now, sin_now = (
                    cos_now * cosine - sin_now * sine,
                    sin_now * cosine + cos_now * sine,
                )
    for z in range(ZBOX):
        for pair in range(YBOX // 2):
            lanes = pl.ds(pair * LANES, LANES)
            even = got_ref[z * YBOX + 2 * pair, :K, :]
            odd = got_ref[z * YBOX + 2 * pair + 1, :K, :]
            state_ref[z, :K, lanes] = jnp.concatenate([even[:, :HALF], odd[:, :HALF]], axis=1)
            state_ref[z, K:, lanes] = jnp.concatenate([even[:, HALF:], odd[:, HALF:]], axis=1)

    def rotated(level, z, lanes, total):
        cosine = cos_ref[level, pl.ds(z, 1), lanes]
        sine = sin_ref[level, pl.ds(z, 1), lanes]
        real, imag = total[:K], total[K:]
        state_ref[z, :K, lanes] = (cosine * real - sine * imag).astype(jnp.bfloat16)
        state_ref[z, K:, lanes] = (sine * real + cosine * imag).astype(jnp.bfloat16)

    for level, bit in ((0, 4), (1, 1), (2, 2)):
        for z in range(ZBOX):
            if z & bit:
                continue
            for part in range(2):
                lanes = pl.ds(part * 256, 256)
                both = jnp.concatenate([state_ref[z, :, lanes], state_ref[z | bit, :, lanes]], 0)
                total = jnp.dot(mats_ref[level], both, preferred_element_type=jnp.float32)
                rotated(level, z, lanes, total[: 2 * K])
                rotated(level, z | bit, lanes, total[2 * K :])
    for z in range(ZBOX):
        first, second = pl.ds(0, 256), pl.ds(256, 256)
        both = jnp.concatenate([state_ref[z, :, first], state_ref[z, :, second]], 0)
        total = jnp.dot(mats_ref[3], both, preferred_element_type=jnp.float32)
        rotated(3, z, first, total[: 2 * K])
        rotated(3, z, second, total[2 * K :])
    for z in range(ZBOX):
        picture_ref[z] = jnp.dot(
            eval_ref[...], state_ref[z], preferred_element_type=jnp.float32
        ).astype(jnp.bfloat16)
    last = place_ref[0] == 7
    first = place_ref[0] == 0
    nothing = jnp.zeros((16, WIDE), jnp.bfloat16)
    for z in range(ZBOX):

        @pl.when(last)
        def _():
            below_ref[z] = picture_ref[z - 2, 48:, :] if z >= 2 else nothing

        @pl.when(jnp.logical_not(last))
        def _():
            below_ref[z] = picture_ref[z, 48:, :]

        @pl.when(first)
        def _():
            above_ref[z] = picture_ref[z + 2, :16, :] if z + 2 < ZBOX else nothing

        @pl.when(jnp.logical_not(first))
        def _():
            above_ref[z] = picture_ref[z, :16, :]


def butterfly(place, got, mats, evaluate):
    whole = pl.BlockSpec(memory_space=pltpu.VMEM)
    return pl.pallas_call(
        butterfly_kernel,
        out_shape=(
            jax.ShapeDtypeStruct((ZBOX, K, WIDE), jnp.bfloat16),
            jax.ShapeDtypeStruct((ZBOX, 16, WIDE), jnp.bfloat16),
            jax.ShapeDtypeStruct((ZBOX, 16, WIDE), jnp.bfloat16),
            jax.ShapeDtypeStruct((ZBOX, WIDE), jnp.float32),
        ),
        in_specs=[pl.BlockSpec(memory_space=pltpu.SMEM), whole, whole, whole],
        out_specs=(whole, whole, whole, whole),
        scratch_shapes=[
            pltpu.VMEM((ZBOX, 2 * K, WIDE), jnp.bfloat16),
            pltpu.VMEM((LEVELS, ZBOX, WIDE), jnp.float32),
            pltpu.VMEM((LEVELS, ZBOX, WIDE), jnp.float32),
        ],
        cost_estimate=pl.CostEstimate(flops=2 << 30, bytes_accessed=3 << 20, transcendentals=8192),
        compiler_params=pltpu.CompilerParams(vmem_limit_bytes=12 << 20),
        name="butterfly",
    )(place, got, mats, evaluate)


def smooth_kernel(picture_ref, below_ref, above_ref, width_ref, sums_ref, out_ref):
    rows = K + 32
    low = lane_low((rows, LANES))
    half_low = lane_low((32, LANES))
    upper = lax.broadcasted_iota(jnp.int32, (rows, LANES), 0) % 8 >= 4
    nothing = jnp.zeros((rows, LANES), jnp.float32)

    def tile(z, pair):
        lanes = pl.ds(pair * LANES, LANES)
        parts = [below_ref[z, :, lanes], picture_ref[z, :, lanes], above_ref[z, :, lanes]]
        return jnp.concatenate(parts, axis=0).astype(jnp.float32)

    for zh in range(ZBOX // 2):
        line = [(2 * zh + i // 4, i % 4) for i in range(8)]
        before, here = nothing, tile(*line[0])
        for i, (z, pair) in enumerate(line):
            after = tile(*line[i + 1]) if i + 1 < len(line) else nothing
            left = jnp.where(low, here, before)
            right = jnp.where(low, after, here)
            beside = turn(jnp.where(upper, left, right))
            field = jnp.concatenate([here, beside], axis=0).astype(jnp.bfloat16)
            sums = jnp.dot(sums_ref[...], field, preferred_element_type=jnp.float32)
            wide = width_ref[pl.ds(z, 1), pl.ds(pair * LANES, LANES)] > 1.5
            chosen = jnp.where(wide, sums[K:] / 25.0, sums[:K] / 9.0)
            top, bottom = chosen[:32], chosen[32:]
            box = z * YBOX + 2 * pair
            out_ref[box] = jnp.where(half_low, top, turn(bottom)).astype(jnp.bfloat16)
            out_ref[box + 1] = jnp.where(half_low, turn(top), bottom).astype(jnp.bfloat16)
            before, here = here, after


def smooth(picture, below, above, widths, sums):
    whole = pl.BlockSpec(memory_space=pltpu.VMEM)
    return pl.pallas_call(
        smooth_kernel,
        out_shape=jax.ShapeDtypeStruct((BOXES, 32, LANES), jnp.bfloat16),
        in_specs=[whole] * 5,
        out_specs=whole,
        cost_estimate=pl.CostEstimate(flops=1 << 28, bytes_accessed=2 << 20, transcendentals=0),
        compiler_params=pltpu.CompilerParams(vmem_limit_bytes=12 << 20),
        name="smooth",
    )(picture, below, above, widths, sums)


def unpack_kernel(got_ref, out_ref):
    for tile in range(out_ref.shape[-1] // LANES):
        lanes = pl.ds(tile * LANES, LANES)
        even = got_ref[2 * tile]
        odd = got_ref[2 * tile + 1]
        out_ref[:32, lanes] = jnp.concatenate([even[:, :HALF], odd[:, :HALF]], axis=1)
        out_ref[32:, lanes] = jnp.concatenate([even[:, HALF:], odd[:, HALF:]], axis=1)


def unpack(got):
    steps = 2
    return pl.pallas_call(
        unpack_kernel,
        grid=(steps,),
        out_shape=jax.ShapeDtypeStruct((K, COLS), jnp.bfloat16),
        in_specs=[pl.BlockSpec((BOXES // steps, 32, LANES), lambda s: (s, 0, 0))],
        out_specs=pl.BlockSpec((K, COLS // steps), lambda s: (0, s)),
        cost_estimate=pl.CostEstimate(flops=1 << 20, bytes_accessed=1 << 20, transcendentals=0),
        compiler_params=pltpu.CompilerParams(vmem_limit_bytes=12 << 20),
        name="unpack",
    )(got)


def box_sums():
    sums = np.zeros((2, TILE, TILE, 2, TILE + 4, TILE), np.float32)
    for reach in (1, 2):
        for a in range(TILE):
            for b in range(TILE):
                for x in range(TILE + 4):
                    for y in range(TILE):
                        if abs(x - 2 - a) > reach:
                            continue
                        other = y - TILE if y >= 4 else y + TILE
                        sums[reach - 1, a, b, 0, x, y] = abs(y - b) <= reach
                        sums[reach - 1, a, b, 1, x, y] = abs(other - b) <= reach
    return sums.reshape(2 * K, 2 * (K + 32))


def blocks(real_part, imag_part):
    upper = jnp.concatenate([real_part, -imag_part], axis=-1)
    lower = jnp.concatenate([imag_part, real_part], axis=-1)
    return jnp.concatenate([upper, lower], axis=-2)


def on_device(
    sources, translate_re, translate_im, frame_index, velocity_index, eval_re, eval_im, window
):
    message = pack(
        window.reshape(1), frame_index.reshape(16), velocity_index.reshape(1, 256), sources[0, 0]
    )
    got = lax.all_to_all(message, GROUP, 0, 0, tiled=True)
    own = blocks(translate_re[:, :, 0], translate_im[:, :, 0])
    other = blocks(translate_re[:, :, 1], translate_im[:, :, 1])
    mats = jnp.concatenate(
        [
            jnp.concatenate([own[:, 0], other[:, 0]], axis=-1),
            jnp.concatenate([other[:, 1], own[:, 1]], axis=-1),
        ],
        axis=-2,
    )
    evaluate = jnp.concatenate([eval_re, -eval_im], axis=1)
    picture, last_rows, first_rows, widths = butterfly(lax.axis_index("xc").reshape(1), got, mats, evaluate)
    below = lax.ppermute(last_rows, "xc", [(i, (i + 1) % 8) for i in range(8)])
    above = lax.ppermute(first_rows, "xc", [(i, (i + 7) % 8) for i in range(8)])
    smoothed = smooth(picture, below, above, widths, jnp.asarray(box_sums(), jnp.bfloat16))
    back = lax.all_to_all(smoothed, GROUP, 0, 0, tiled=True)
    return unpack(back).reshape(TILE, TILE, COLS)


def solution(mesh):
    fine = Mesh(mesh.devices.reshape(4, 8, 2, 8), ("zh", "xc", "zl", "y"))
    box = (("zh", "xc"), ("zl", "y"))
    return jax.shard_map(
        on_device,
        mesh=fine,
        in_specs=(
            P(*box, None, None, None),
            P(),
            P(),
            P(*box, None),
            P(*box, None),
            P(),
            P(),
            P(*box),
        ),
        out_specs=P(*box, None),
        check_vma=False,
    )
```
